32 devices in a mesh: grp: 2 (over x), row: 16 (over z, y, core).
Axes of the slice: x: 2, y: 2, z: 4, core: 2. Of those that a mesh axis runs over, the one named last changes fastest.
Arguments:
- kmesh: int32 [32, 3], P(('grp', 'row')), parts along dimension 0, may hold values from 0 to 15
- rcoord: int32 [768, 3], P(('grp', 'row')), parts along dimension 0, may hold values from -8 to 8
- degen: int32 [768], P(('grp', 'row')), parts along dimension 0, may hold values from 1 to 4
- hr_re: float32 [768, 128, 128], P(('grp', 'row')), parts along dimension 0, may hold values from -1.5 to 1.5
- hr_im: float32 [768, 128, 128], P(('grp', 'row')), parts along dimension 0, may hold values from -1.5 to 1.5
Outputs:
- hk_re: float32 [32, 128, 128], P(('grp', 'row')), parts along dimension 0
- hk_im: float32 [32, 128, 128], P(('grp', 'row')), parts along dimension 0
The draws below stay inside these ranges and needn't reach their ends.
There are 2 independent parts, one for each index of `grp`. The reference program is written for one: setup_inputs(seed, part) draws one part's arguments, and reference() takes and returns one part's arrays. A program takes and returns all parts, laid end to end along the dimension named above; each array names one. Nothing has to cross between parts.
All inputs are finite; a program needn't handle non-finite values.
Results may differ from the reference program's by a relative error of at most 0.00007.
Values sent between devices are 32-bit elements; how exact they have to be, the bound alone decides.
No kernel may reach another device: no remote copies, remote signals or barrier semaphores. Data moves between devices by JAX's collectives and lax.ppermute only.
A program may use at most 64 MiB of HBM per device.

```python
import math
import jax
import jax.numpy as jnp
from jax import lax

NW = 128
MESH = 16
NR = 384
K = 16


def place_ends(entries, stream_key, low, high):
    longest = entries.shape.index(max(entries.shape))
    spots = []
    for shift in (0, 1):
        where = [jax.random.randint(jax.random.fold_in(stream_key, axis), (), 0, length) for axis, length in enumerate(entries.shape)]
        where[longest] = (where[longest] + shift) % entries.shape[longest]
        spots.append(tuple(where))
    return entries.at[spots[0]].set(low).at[spots[1]].set(high)


def block_levels(stream_key, dims, cuts, smallest, high):
    factor_of, own = 1.0, jax.random.fold_in(stream_key, 6)
    for position, parts in cuts:
        steps = jnp.exp(jax.random.uniform(jax.random.fold_in(own, position), (parts,), jnp.float32, smallest / len(cuts), high / len(cuts)))
        factor_of = factor_of * jnp.repeat(steps, dims[position] // parts).reshape([-1 if axis == position else 1 for axis in range(len(dims))])
    return factor_of


def scatter_about(own_key, shape, scale, most, shards=(), kind=jnp.bfloat16):
    values = jax.random.normal(own_key, shape, jnp.float32) * scale
    if len(shards) > 0:
        values = block_levels(own_key, shape, shards, -0.22, 0.18) * values
    return jnp.clip(values, min=-most, max=most).astype(kind)


def setup_inputs(seed: int = 0, part: int = 0) -> dict:
    arg_keys = jax.random.split(jax.random.key(seed), 6)
    part_keys = jax.random.split(jax.random.fold_in(arg_keys[5], part), 6)
    return {
        "kmesh": place_ends(jax.random.randint(part_keys[0], (K, 3), 0, MESH), jax.random.fold_in(part_keys[0], 1), 0, MESH - 1).astype(jnp.int32),
        "rcoord": place_ends(jax.random.randint(part_keys[1], (NR, 3), -8, 9), jax.random.fold_in(part_keys[1], 1), -8, 8).astype(jnp.int32),
        "degen": place_ends(jax.random.randint(part_keys[2], (NR,), 1, 5), jax.random.fold_in(part_keys[2], 1), 1, 4).astype(jnp.int32),
        "hr_re": scatter_about(part_keys[3], (NR, NW, NW), (2.0 / NR ** 0.5), 1.5, ((0, 16),), jnp.float32),
        "hr_im": scatter_about(part_keys[4], (NR, NW, NW), (2.0 / NR ** 0.5), 1.5, ((0, 16),), jnp.float32),
    }


def reference(kmesh, rcoord, degen, hr_re, hr_im):
    prod = jnp.sum(kmesh[:, None, :] * rcoord[None, :, :], axis=-1)
    phase = jnp.mod(prod, MESH).astype(jnp.int32)
    angle = phase.astype(jnp.float32) * (2.0 * math.pi / MESH)
    inverse = 1.0 / degen.astype(jnp.float32)
    cosine = jnp.cos(angle) * inverse[None, :]
    sine = jnp.sin(angle) * inverse[None, :]
    real_flat = hr_re.reshape(hr_re.shape[0], -1)
    imag_flat = hr_im.reshape(hr_im.shape[0], -1)
    hi = lax.Precision.HIGHEST
    out_re = jnp.dot(cosine, real_flat, precision=hi, preferred_element_type=jnp.float32) - jnp.dot(sine, imag_flat, precision=hi, preferred_element_type=jnp.float32)
    out_im = jnp.dot(sine, real_flat, precision=hi, preferred_element_type=jnp.float32) + jnp.dot(cosine, imag_flat, precision=hi, preferred_element_type=jnp.float32)
    width = hr_re.shape[1]
    return out_re.reshape(-1, width, width), out_im.reshape(-1, width, width)
```

```python
import functools
import math

import jax
import jax.numpy as jnp
from jax import lax
from jax.experimental import pallas as pl
from jax.experimental.pallas import tpu as pltpu
from jax.sharding import PartitionSpec as P

MESH = 16
SUB = 8


def swap(x, distance, count):
    return lax.ppermute(x, "row", [(i, i ^ distance) for i in range(count)])


def split_bf16(x):
    high = x.astype(jnp.bfloat16)
    low = (x - high.astype(jnp.float32)).astype(jnp.bfloat16)
    return high, low


def onehot(shape, match):
    first = lax.broadcasted_iota(jnp.int32, shape, 0)
    second = lax.broadcasted_iota(jnp.int32, shape, 1)
    return match(first, second)


def dot(a, b):
    return lax.dot_general(a, b, (((1,), (0,)), ((), ())), preferred_element_type=jnp.float32)


def fourier_kernel(coef_ref, re_ref, im_ref, re2_ref, im2_ref,
                   are_keep, are_send, aim_keep, aim_send, high_ref, both_ref):
    rows, cols = coef_ref.shape
    big_rows, big_cols = rows * SUB, cols * SUB

    @pl.when(pl.program_id(0) == 0)
    def _():
        spread_r = onehot((big_rows, rows), lambda i, j: i // SUB == j).astype(jnp.bfloat16)
        spread_c = onehot((cols, big_cols), lambda i, j: j // SUB == i).astype(jnp.bfloat16)
        diagonal = onehot((big_rows, big_cols), lambda i, j: i % SUB == j % SUB)
        for part, base in zip(split_bf16(coef_ref[...]), (0, big_rows)):
            wide = dot(spread_r, part).astype(jnp.bfloat16)
            full = jnp.where(diagonal, dot(wide, spread_c), 0.0).astype(jnp.bfloat16)
            both_ref[base:base + big_rows, :] = full
            if base == 0:
                high_ref[...] = full

    tiles = re_ref.shape[1] // SUB
    lanes = re_ref.shape[2]
    quarter = big_rows // 4
    outs = (are_keep, are_send, aim_keep, aim_send)
    for pair in range(0, tiles, 2):
        columns = []
        for t in (pair, pair + 1):
            span = slice(t * SUB, (t + 1) * SUB)
            columns.append(jnp.concatenate(
                [ref[:, span, :].reshape(-1, lanes) for ref in (re_ref, re2_ref, im_ref, im2_ref)], axis=0))
        x_high, x_low = split_bf16(jnp.concatenate(columns, axis=1))
        first = dot(both_ref[...], x_high)
        total = first[:big_rows] + first[big_rows:] + dot(high_ref[...], x_low)
        for which, t in enumerate((pair, pair + 1)):
            span = slice(t * SUB, (t + 1) * SUB)
            for part, ref in enumerate(outs):
                piece = total[part * quarter:(part + 1) * quarter, which * lanes:(which + 1) * lanes]
                ref[:, span, :] = piece.reshape(-1, SUB, lanes)


def transform(coef, re, im, re2, im2):
    rows, cols = coef.shape
    local_r, height, width = re.shape
    step = 32
    half_k = rows // 4
    block = pl.BlockSpec((local_r, step, width), lambda i: (0, i, 0))
    out = pl.BlockSpec((half_k, step, width), lambda i: (0, i, 0))
    return pl.pallas_call(
        fourier_kernel,
        grid=(height // step,),
        in_specs=[pl.BlockSpec((rows, cols), lambda i: (0, 0))] + [block] * 4,
        out_specs=[out] * 4,
        out_shape=[jax.ShapeDtypeStruct((half_k, height, width), jnp.float32)] * 4,
        scratch_shapes=[
            pltpu.VMEM((rows * SUB, cols * SUB), jnp.bfloat16),
            pltpu.VMEM((2 * rows * SUB, cols * SUB), jnp.bfloat16),
        ],
        name="fourier",
    )(coef, re, im, re2, im2)


def coefficients(k, coords, inverse):
    prod = jnp.sum(k[:, None, :] * coords[None, :, :], axis=-1)
    angle = jnp.mod(prod, MESH).astype(jnp.float32) * (2.0 * math.pi / MESH)
    return jnp.cos(angle) * inverse[None, :], jnp.sin(angle) * inverse[None, :]


def ordered(k, bits, order):
    cube = k.reshape((2,) * len(bits) + (k.shape[1],))
    axes = tuple(len(bits) - 1 - bits.index(b) for b in order)
    return cube.transpose(axes + (len(bits),)).reshape(k.shape)


def shards(kmesh, rcoord, degen, hr_re, hr_im, count):
    swap_n = functools.partial(swap, count=count)
    bits = [1 << b for b in range(1, count.bit_length() - 1)]
    re2 = swap_n(hr_re, 1)
    im2 = swap_n(hr_im, 1)
    table = jnp.concatenate([rcoord, degen[:, None]], axis=1)
    table = jnp.concatenate([table, swap_n(table, 1)], axis=0)
    k = kmesh
    for b in bits:
        k = jnp.concatenate([k, swap_n(k, b)], axis=0)
    order_a = list(bits)
    order_b = [bits[1], bits[0]] + bits[2:]
    inverse = 1.0 / table[:, 3].astype(jnp.float32)
    cos_a, sin_a = coefficients(ordered(k, bits, order_a), table[:, :3], inverse)
    cos_b, sin_b = coefficients(ordered(k, bits, order_b), table[:, :3], inverse)
    coef = jnp.concatenate([
        jnp.concatenate([cos_a, -sin_a], axis=1),
        jnp.concatenate([sin_b, cos_b], axis=1),
    ], axis=0)
    a, a_send, b, b_send = transform(coef, hr_re, hr_im, re2, im2)
    for stage, (bit_a, bit_b) in enumerate(zip(order_a, order_b)):
        a = a + swap_n(a_send, bit_a)
        b = b + swap_n(b_send, bit_b)
        if stage + 1 < len(bits):
            half = a.shape[0] // 2
            a, a_send = a[:half], a[half:]
            b, b_send = b[:half], b[half:]
    return a, b


def solution(mesh):
    rows = P(("grp", "row"))
    placed = (
        P(("grp", "row"), None),
        P(("grp", "row"), None),
        rows,
        P(("grp", "row"), None, None),
        P(("grp", "row"), None, None),
    )
    return jax.shard_map(
        functools.partial(shards, count=mesh.shape["row"]),
        mesh=mesh,
        in_specs=placed,
        out_specs=(P(("grp", "row"), None, None), P(("grp", "row"), None, None)),
        check_vma=False,
    )
```

```python
import functools
import math

import jax
import jax.numpy as jnp
from jax import lax
from jax.experimental import pallas as pl
from jax.experimental.pallas import tpu as pltpu
from jax.sharding import PartitionSpec as P

MESH = 16
SUB = 8


def swap(x, distance, count):
    return lax.ppermute(x, "row", [(i, i ^ distance) for i in range(count)])


def split_bf16(x):
    high = x.astype(jnp.bfloat16)
    low = (x - high.astype(jnp.float32)).astype(jnp.bfloat16)
    return high, low


def onehot(shape, match):
    first = lax.broadcasted_iota(jnp.int32, shape, 0)
    second = lax.broadcasted_iota(jnp.int32, shape, 1)
    return match(first, second)


def dot(a, b):
    return lax.dot_general(a, b, (((1,), (0,)), ((), ())), preferred_element_type=jnp.float32)


def prepare_kernel(re_ref, im_ref, high_ref, low_ref):
    lanes = re_ref.shape[2]
    columns = []
    for t in range(re_ref.shape[1] // SUB):
        span = slice(t * SUB, (t + 1) * SUB)
        columns.append(jnp.concatenate(
            [ref[:, span, :].reshape(-1, lanes) for ref in (re_ref, im_ref)], axis=0))
    high_ref[0], low_ref[0] = split_bf16(jnp.concatenate(columns, axis=1))


def prepare(re, im):
    local_r, height, width = re.shape
    step = 2 * SUB
    block = pl.BlockSpec((local_r, step, width), lambda i: (0, i, 0))
    shape = (height // step, 2 * local_r * SUB, 2 * width)
    out = pl.BlockSpec((1,) + shape[1:], lambda i: (i, 0, 0))
    return pl.pallas_call(
        prepare_kernel,
        grid=(height // step,),
        in_specs=[block] * 2,
        out_specs=[out] * 2,
        out_shape=[jax.ShapeDtypeStruct(shape, jnp.bfloat16)] * 2,
        compiler_params=pltpu.CompilerParams(vmem_limit_bytes=8 << 20),
        name="prepare",
    )(re, im)


def fetch_kernel(re_ref, im_ref, high_ref, low_ref, re_buf, im_buf, sems):
    steps = high_ref.shape[0]
    step = re_ref.shape[1] // steps
    copies = []
    for i in range(steps):
        span = pl.ds(i * step, step)
        copies.append([pltpu.make_async_copy(src.at[:, span, :], dst.at[:, span, :], sems.at[which, i])
                       for which, (src, dst) in enumerate(((re_ref, re_buf), (im_ref, im_buf)))])
        for copy in copies[i]:
            copy.start()
    lanes = re_ref.shape[2]
    for i in range(steps):
        for copy in copies[i]:
            copy.wait()
        columns = []
        for t in range(i * step, (i + 1) * step, SUB):
            columns.append(jnp.concatenate(
                [buf[:, t:t + SUB, :].reshape(-1, lanes) for buf in (re_buf, im_buf)], axis=0))
        high_ref[i], low_ref[i] = split_bf16(jnp.concatenate(columns, axis=1))


def fetch(re, im):
    local_r, height, width = re.shape
    steps = height // (2 * SUB)
    shape = (steps, 2 * local_r * SUB, 2 * width)
    return pl.pallas_call(
        fetch_kernel,
        in_specs=[pl.BlockSpec(memory_space=pltpu.HBM)] * 2,
        out_specs=[pl.BlockSpec(memory_space=pltpu.VMEM)] * 2,
        out_shape=[jax.ShapeDtypeStruct(shape, jnp.bfloat16)] * 2,
        scratch_shapes=[pltpu.VMEM(re.shape, jnp.float32)] * 2 + [pltpu.SemaphoreType.DMA((2, steps))],
        compiler_params=pltpu.CompilerParams(vmem_limit_bytes=57 << 20),
        name="fetch",
    )(re, im)


def gathered(place, bits, swapped):
    index = jnp.zeros_like(place)
    for turn in range(len(bits)):
        bit = (place >> (len(bits) - 1 - turn)) & 1
        index = index + (bit << ({0: 1, 1: 0}.get(turn, turn) if swapped else turn))
    return index


def fourier_kernel(bits, send, k_ref, coords_ref, degen_ref, coords2_ref, degen2_ref,
                   high1_ref, low1_ref, high2_ref, low2_ref, a_ref, b_ref, both1_ref, both2_ref):
    count = k_ref.shape[0]
    half = count // 2
    local_r = coords_ref.shape[1]
    rows, cols = 2 * half * SUB, 2 * local_r * SUB
    group = lax.broadcasted_iota(jnp.int32, (rows, 2 * count), 0) // SUB
    column = lax.broadcasted_iota(jnp.int32, (rows, 2 * count), 1)
    is_b = group >= half
    place = group % half + (half if send else 0)
    index = jnp.where(is_b, gathered(place, bits, True), gathered(place, bits, False))
    other = index + count
    pick0 = jnp.where(jnp.where(is_b, other, index) == column, 1.0, 0.0).astype(jnp.bfloat16)
    sign = jnp.where(is_b, 1.0, -1.0)
    pick1 = jnp.where(jnp.where(is_b, index, other) == column, sign, 0.0).astype(jnp.bfloat16)
    diagonal = onehot((rows, cols), lambda i, j: i % SUB == j % SUB)
    spread = [onehot((local_r, cols), lambda i, j: j // SUB == i + q * local_r)
              .astype(jnp.float32).astype(jnp.bfloat16) for q in (0, 1)]
    sides = ((coords_ref, degen_ref, both1_ref), (coords2_ref, degen2_ref, both2_ref))
    for coords, degen, both in sides:
        prod = sum(k_ref[:, d:d + 1] * coords[d:d + 1, :] for d in range(coords.shape[0]))
        angle = (prod & (MESH - 1)).astype(jnp.float32) * (2.0 * math.pi / MESH)
        inverse = 1.0 / degen[...].astype(jnp.float32)
        table = jnp.concatenate([jnp.cos(angle) * inverse, jnp.sin(angle) * inverse], axis=0)
        for level, part in enumerate(split_bf16(table)):
            full = sum(dot(dot(pick, part).astype(jnp.bfloat16), wide)
                       for pick, wide in zip((pick0, pick1), spread))
            both[level * rows:(level + 1) * rows, :] = jnp.where(diagonal, full, 0.0).astype(jnp.bfloat16)

    pairs, _, width2 = high1_ref.shape
    lanes = width2 // 2
    for pair in range(pairs):
        first = dot(both1_ref[...], high1_ref[pair]) + dot(both2_ref[...], high2_ref[pair])
        total = dot(both1_ref[:rows], low1_ref[pair]) + dot(both2_ref[:rows], low2_ref[pair])
        total = total + first[rows:] + first[:rows]
        for which in (0, 1):
            span = slice((2 * pair + which) * SUB, (2 * pair + which + 1) * SUB)
            for part, ref in enumerate((a_ref, b_ref)):
                piece = total[part * half * SUB:(part + 1) * half * SUB, which * lanes:(which + 1) * lanes]
                ref[:, span, :] = piece.reshape(half, SUB, lanes)


def transform(bits, send, k, small, own, peer, shape):
    half = k.shape[0] // 2
    local_r = small[0].shape[1]
    operands = [k, *small, *own, *peer]
    vmem = pl.BlockSpec(memory_space=pltpu.VMEM)
    scratch = pltpu.VMEM((4 * half * SUB, 2 * local_r * SUB), jnp.bfloat16)
    return pl.pallas_call(
        functools.partial(fourier_kernel, bits, send),
        in_specs=[vmem] * len(operands),
        out_specs=[vmem] * 2,
        out_shape=[jax.ShapeDtypeStruct((half,) + shape, jnp.float32)] * 2,
        scratch_shapes=[scratch] * 2,
        compiler_params=pltpu.CompilerParams(vmem_limit_bytes=32 << 20),
        name="fourier_send" if send else "fourier_keep",
    )(*operands)


def shards(kmesh, rcoord, degen, hr_re, hr_im, count):
    swap_n = functools.partial(swap, count=count)
    bits = [1 << b for b in range(1, count.bit_length() - 1)]
    re2 = swap_n(hr_re, 1)
    im2 = swap_n(hr_im, 1)
    coords = rcoord.T
    weights = degen[None, :]
    coords2 = swap_n(coords, 1)
    weights2 = swap_n(weights, 1)
    k = kmesh
    for b in bits:
        k = jnp.concatenate([k, swap_n(k, b)], axis=0)
    order_a = list(bits)
    order_b = [bits[1], bits[0]] + bits[2:]
    small = (coords, weights, coords2, weights2)
    own = fetch(hr_re, hr_im)
    peer = prepare(re2, im2)
    a_send, b_send = transform(bits, True, k, small, own, peer, hr_re.shape[1:])
    a, b = transform(bits, False, k, small, own, peer, hr_re.shape[1:])
    for stage, (bit_a, bit_b) in enumerate(zip(order_a, order_b)):
        a = a + swap_n(a_send, bit_a)
        b = b + swap_n(b_send, bit_b)
        if stage + 1 < len(bits):
            half = a.shape[0] // 2
            a, a_send = a[:half], a[half:]
            b, b_send = b[:half], b[half:]
    return a, b


def solution(mesh):
    rows = P(("grp", "row"))
    placed = (
        P(("grp", "row"), None),
        P(("grp", "row"), None),
        rows,
        P(("grp", "row"), None, None),
        P(("grp", "row"), None, None),
    )
    return jax.shard_map(
        functools.partial(shards, count=mesh.shape["row"]),
        mesh=mesh,
        in_specs=placed,
        out_specs=(P(("grp", "row"), None, None), P(("grp", "row"), None, None)),
        check_vma=False,
    )
```

```python
import functools
import math

import jax
import jax.numpy as jnp
from jax import lax
from jax.experimental import pallas as pl
from jax.experimental.pallas import tpu as pltpu
from jax.sharding import PartitionSpec as P

MESH = 16
SUB = 8


def swap(x, distance, count):
    return lax.ppermute(x, "row", [(i, i ^ distance) for i in range(count)])


def split_bf16(x):
    high = x.astype(jnp.bfloat16)
    low = (x - high.astype(jnp.float32)).astype(jnp.bfloat16)
    return high, low


def onehot(shape, match):
    first = lax.broadcasted_iota(jnp.int32, shape, 0)
    second = lax.broadcasted_iota(jnp.int32, shape, 1)
    return match(first, second)


def dot(a, b):
    return lax.dot_general(a, b, (((1,), (0,)), ((), ())), preferred_element_type=jnp.float32)


def prepare_kernel(re_ref, im_ref, high_ref, low_ref):
    lanes = re_ref.shape[2]
    columns = []
    for t in range(re_ref.shape[1] // SUB):
        span = slice(t * SUB, (t + 1) * SUB)
        columns.append(jnp.concatenate(
            [ref[:, span, :].reshape(-1, lanes) for ref in (re_ref, im_ref)], axis=0))
    high_ref[0], low_ref[0] = split_bf16(jnp.concatenate(columns, axis=1))


def prepare(re, im):
    local_r, height, width = re.shape
    step = 2 * SUB
    block = pl.BlockSpec((local_r, step, width), lambda i: (0, i, 0))
    shape = (height // step, 2 * local_r * SUB, 2 * width)
    out = pl.BlockSpec((1,) + shape[1:], lambda i: (i, 0, 0))
    return pl.pallas_call(
        prepare_kernel,
        grid=(height // step,),
        in_specs=[block] * 2,
        out_specs=[out] * 2,
        out_shape=[jax.ShapeDtypeStruct(shape, jnp.bfloat16)] * 2,
        compiler_params=pltpu.CompilerParams(vmem_limit_bytes=8 << 20),
        name="prepare",
    )(re, im)


def gathered(place, bits, swapped):
    index = jnp.zeros_like(place)
    for turn in range(len(bits)):
        bit = (place >> (len(bits) - 1 - turn)) & 1
        index = index + (bit << ({0: 1, 1: 0}.get(turn, turn) if swapped else turn))
    return index


def fourier_kernel(bits, send, k_ref, coords_ref, degen_ref, coords2_ref, degen2_ref,
                   high1_ref, low1_ref, high2_ref, low2_ref, a_ref, b_ref, both1_ref, both2_ref):
    count = k_ref.shape[0]
    half = count // 2
    local_r = coords_ref.shape[1]
    rows, cols = 2 * half * SUB, 2 * local_r * SUB
    group = lax.broadcasted_iota(jnp.int32, (rows, 2 * count), 0) // SUB
    column = lax.broadcasted_iota(jnp.int32, (rows, 2 * count), 1)
    is_b = group >= half
    place = group % half + (half if send else 0)
    index = jnp.where(is_b, gathered(place, bits, True), gathered(place, bits, False))
    other = index + count
    pick0 = jnp.where(jnp.where(is_b, other, index) == column, 1.0, 0.0).astype(jnp.bfloat16)
    sign = jnp.where(is_b, 1.0, -1.0)
    pick1 = jnp.where(jnp.where(is_b, index, other) == column, sign, 0.0).astype(jnp.bfloat16)
    diagonal = onehot((rows, cols), lambda i, j: i % SUB == j % SUB)
    spread = [onehot((local_r, cols), lambda i, j: j // SUB == i + q * local_r)
              .astype(jnp.float32).astype(jnp.bfloat16) for q in (0, 1)]
    sides = ((coords_ref, degen_ref, both1_ref), (coords2_ref, degen2_ref, both2_ref))
    for coords, degen, both in sides:
        prod = sum(k_ref[:, d:d + 1] * coords[d:d + 1, :] for d in range(coords.shape[0]))
        angle = (prod & (MESH - 1)).astype(jnp.float32) * (2.0 * math.pi / MESH)
        inverse = 1.0 / degen[...].astype(jnp.float32)
        table = jnp.concatenate([jnp.cos(angle) * inverse, jnp.sin(angle) * inverse], axis=0)
        for level, part in enumerate(split_bf16(table)):
            full = sum(dot(dot(pick, part).astype(jnp.bfloat16), wide)
                       for pick, wide in zip((pick0, pick1), spread))
            both[level * rows:(level + 1) * rows, :] = jnp.where(diagonal, full, 0.0).astype(jnp.bfloat16)

    pairs, _, width2 = high1_ref.shape
    lanes = width2 // 2
    for pair in range(pairs):
        first = dot(both1_ref[...], high1_ref[pair]) + dot(both2_ref[...], high2_ref[pair])
        total = dot(both1_ref[:rows], low1_ref[pair]) + dot(both2_ref[:rows], low2_ref[pair])
        total = total + first[rows:] + first[:rows]
        for which in (0, 1):
            span = slice((2 * pair + which) * SUB, (2 * pair + which + 1) * SUB)
            for part, ref in enumerate((a_ref, b_ref)):
                piece = total[part * half * SUB:(part + 1) * half * SUB, which * lanes:(which + 1) * lanes]
                ref[:, span, :] = piece.reshape(half, SUB, lanes)


def transform(bits, send, k, small, own, peer, shape):
    half = k.shape[0] // 2
    local_r = small[0].shape[1]
    operands = [k, *small, *own, *peer]
    vmem = pl.BlockSpec(memory_space=pltpu.VMEM)
    scratch = pltpu.VMEM((4 * half * SUB, 2 * local_r * SUB), jnp.bfloat16)
    return pl.pallas_call(
        functools.partial(fourier_kernel, bits, send),
        in_specs=[vmem] * len(operands),
        out_specs=[vmem] * 2,
        out_shape=[jax.ShapeDtypeStruct((half,) + shape, jnp.float32)] * 2,
        scratch_shapes=[scratch] * 2,
        compiler_params=pltpu.CompilerParams(vmem_limit_bytes=32 << 20),
        name="fourier_send" if send else "fourier_keep",
    )(*operands)


def shards(kmesh, rcoord, degen, hr_re, hr_im, count):
    swap_n = functools.partial(swap, count=count)
    bits = [1 << b for b in range(1, count.bit_length() - 1)]
    re2 = swap_n(hr_re, 1)
    im2 = swap_n(hr_im, 1)
    coords = rcoord.T
    weights = degen[None, :]
    coords2 = swap_n(coords, 1)
    weights2 = swap_n(weights, 1)
    k = kmesh
    for b in bits:
        if b == bits[-1]:
            k, re1, im1, re2, im2 = lax.optimization_barrier((k, hr_re, hr_im, re2, im2))
        k = lax.optimization_barrier(jnp.concatenate([k, swap_n(k, b)], axis=0))
    order_a = list(bits)
    order_b = [bits[1], bits[0]] + bits[2:]
    small = (coords, weights, coords2, weights2)
    own = prepare(re1, im1)
    peer = prepare(re2, im2)
    a_send, b_send = transform(bits, True, k, small, own, peer, hr_re.shape[1:])
    a, b = transform(bits, False, k, small, own, peer, hr_re.shape[1:])
    for stage, (bit_a, bit_b) in enumerate(zip(order_a, order_b)):
        a = a + swap_n(a_send, bit_a)
        b = b + swap_n(b_send, bit_b)
        if stage + 1 < len(bits):
            half = a.shape[0] // 2
            a, a_send = a[:half], a[half:]
            b, b_send = b[:half], b[half:]
    return a, b


def solution(mesh):
    rows = P(("grp", "row"))
    placed = (
        P(("grp", "row"), None),
        P(("grp", "row"), None),
        rows,
        P(("grp", "row"), None, None),
        P(("grp", "row"), None, None),
    )
    return jax.shard_map(
        functools.partial(shards, count=mesh.shape["row"]),
        mesh=mesh,
        in_specs=placed,
        out_specs=(P(("grp", "row"), None, None), P(("grp", "row"), None, None)),
        check_vma=False,
    )
```
